32 devices in a mesh: group: 2 (over core), node: 4 (over y, x), chip: 4 (over z).
Axes of the slice: x: 2, y: 2, z: 4, core: 2. Of those that a mesh axis runs over, the one named last changes fastest.
Arguments:
- prompt_cache: bfloat16 [2, 4, 4, 96, 576], P('group', 'node', None, 'chip'), may hold values from -4 to 4
- prompt_lengths: int32 [2, 4, 4], replicated, may hold values from 1 to 96, 240 in all within a row
- prompt_replica: int32 [2, 4, 4], replicated, may hold values from 0 to 3, as said below
- new_queries: bfloat16 [2, 4, 4, 2, 128, 576], P('group', 'node', None, None, 'chip'), may hold values from -32 to 32
- new_rows: bfloat16 [2, 4, 4, 2, 576], P('group', 'node'), may hold values from -4 to 4
- resident_cache: bfloat16 [2, 4, 3, 1024, 576], P('group', 'node'), may hold values from -4 to 4
- resident_queries: bfloat16 [2, 4, 3, 2, 128, 576], P('group', 'node', None, None, 'chip'), may hold values from -32 to 32
- resident_rows: bfloat16 [2, 4, 3, 2, 576], P('group', 'node'), may hold values from -4 to 4
- resident_lengths: int32 [2, 4, 3], P('group', 'node'), may hold values from 1 to 1024, 1920 in all within a row
Outputs:
- new_context: bfloat16 [2, 4, 4, 2, 128, 512], P('group', 'node', None, None, 'chip')
- resident_context: bfloat16 [2, 4, 3, 2, 128, 512], P('group', 'node', None, None, 'chip')
The draws below stay inside these ranges and needn't reach their ends.
Inputs may be any that keep to these rules, and one draw needn't show every extreme that they name: `prompt_replica`: the 4 prompts of one prefill node go to different replicas; one replica may receive prompts from any number of prefill nodes.
All inputs are finite; a program needn't handle non-finite values.
Results may differ from the reference program's by a relative error of at most 0.0034.
Values may be sent and summed in bfloat16 or wider, within the bound.
A program may use at most 64 MiB of HBM per device.

```python
import math
import jax
import jax.numpy as jnp
import numpy as np
from jax import lax

HEADS = 128
LATENT = 512
CW = 576
STEPS = 2
LEN = 96
PRN = 4
RES = 3
RLEN = 1024
N_GROUP = 2
N_NODE = 4


def latent_values(seed_key, array_shape):
    return jnp.clip(jax.random.normal(seed_key, array_shape, jnp.float32), -4.0, 4.0)


def first_rows(seed_key, lead_shape):
    return latent_values(jax.random.fold_in(seed_key, 1), lead_shape + (1, CW))


def cache_with_first(seed_key, lead_shape, row_count):
    first_row = first_rows(seed_key, lead_shape)
    later_rows = latent_values(jax.random.fold_in(seed_key, 2), lead_shape + (row_count - 1, CW))
    return jnp.concatenate([first_row, later_rows], axis=-2)


def replica_table(seed_key):
    jitter_key, favour_key = jax.random.split(seed_key)
    jitter = jax.random.randint(jitter_key, (N_GROUP, N_NODE, N_NODE), 0, 2 ** 20)
    favour = jax.random.randint(favour_key, (N_GROUP, 1, N_NODE), 0, 3) * 2 ** 19
    scores = (jitter + favour) * N_NODE + lax.broadcasted_iota(jnp.int32, (N_GROUP, N_NODE, N_NODE), 2)
    ranked = jnp.argsort(-scores, axis=-1)
    return ranked[..., :PRN].astype(jnp.int32)


def draw_prompt_cache(key, part):
    return cache_with_first(jax.random.fold_in(key, 11), (N_GROUP, N_NODE, PRN), LEN).astype(jnp.bfloat16)


def draw_prompt_replica(key, part):
    return replica_table(jax.random.fold_in(key, 7))


def draw_new_rows(key, part):
    return latent_values(jax.random.fold_in(key, 41), (N_GROUP, N_NODE, N_NODE, STEPS, CW)).astype(jnp.bfloat16)


def draw_new_queries(key, part):
    drawn_part = jnp.clip(jax.random.normal(jax.random.fold_in(key, 31), (N_GROUP, N_NODE, N_NODE, STEPS, HEADS, CW), jnp.float32), -4.0, 4.0)
    return drawn_part.astype(jnp.bfloat16)


def draw_resident_cache(key, part):
    return cache_with_first(jax.random.fold_in(key, 51), (N_GROUP, N_NODE, RES), RLEN).astype(jnp.bfloat16)


def draw_resident_rows(key, part):
    return latent_values(jax.random.fold_in(key, 61), (N_GROUP, N_NODE, RES, STEPS, CW)).astype(jnp.bfloat16)


def draw_resident_queries(key, part):
    drawn_part = jnp.clip(jax.random.normal(jax.random.fold_in(key, 71), (N_GROUP, N_NODE, RES, STEPS, HEADS, CW), jnp.float32), -4.0, 4.0)
    return drawn_part.astype(jnp.bfloat16)


def length_profile(amount, total, reach, skew):
    loads = [(1 << 20) // math.isqrt(rank ** skew) + 1 for rank in range(2, amount + 1)]
    surplus, holding = total - reach - (amount - 1), [1] * (amount - 1)
    while surplus > 0:
        movable = [i for i in range(amount - 1) if holding[i] < reach]
        mass, remaining = sum([loads[i] for i in movable]), surplus
        for i in movable:
            more = min(reach - holding[i], max(1, remaining * loads[i] // mass), surplus)
            holding[i] = holding[i] + more
            surplus = surplus - more
    return np.array([reach] + holding)


def uneven_parts(key, count, total, bound, slope):
    if count == 2:
        one = jax.random.randint(key, (), max(1, total - bound), min(bound, total - 1) + 1)
        return jnp.stack([one, total - one])
    sizes = jnp.asarray(length_profile(count, total, bound, slope), jnp.int32)
    twos = (count - 1) // 2
    giver, receiver = sizes[1:1 + 2 * twos:2], sizes[2:2 + 2 * twos:2]
    margin = jnp.minimum(giver - 1, bound - receiver)
    shifted = jax.random.randint(jax.random.fold_in(key, 1), (twos,), 0, 1 << 20) % (margin + 1)
    sizes = sizes.at[1:1 + 2 * twos:2].set(giver - shifted).at[2:2 + 2 * twos:2].set(receiver + shifted)
    return sizes[jax.random.permutation(jax.random.fold_in(key, 2), count)]


def setup_inputs(seed: int = 0) -> dict:
    splits = jax.random.split(jax.random.key(seed), 10)
    return {
        "prompt_cache": draw_prompt_cache(jax.random.fold_in(splits[9], 71), 0),
        "prompt_lengths": jax.vmap(lambda own: uneven_parts(own, PRN, PRN * LEN * 5 // 8, LEN, 1))(jax.random.split(splits[1], N_GROUP * N_NODE)).reshape((N_GROUP, N_NODE, PRN)).astype(jnp.int32),
        "prompt_replica": draw_prompt_replica(jax.random.fold_in(splits[9], 71), 0),
        "new_queries": draw_new_queries(jax.random.fold_in(splits[9], 71), 0),
        "new_rows": draw_new_rows(jax.random.fold_in(splits[9], 71), 0),
        "resident_cache": draw_resident_cache(jax.random.fold_in(splits[9], 71), 0),
        "resident_queries": draw_resident_queries(jax.random.fold_in(splits[9], 71), 0),
        "resident_rows": draw_resident_rows(jax.random.fold_in(splits[9], 71), 0),
        "resident_lengths": jax.vmap(lambda own: uneven_parts(own, RES, RES * RLEN * 5 // 8, RLEN, 1))(jax.random.split(splits[8], N_GROUP * N_NODE)).reshape((N_GROUP, N_NODE, RES)).astype(jnp.int32),
    }


score_scale = 1.0 / 192.0 ** 0.5


def scores_of(queries, keys_block):
    return jnp.einsum("bshc,blc->bshl", queries.astype(jnp.float32), keys_block.astype(jnp.float32), precision=lax.Precision.HIGHEST) * score_scale


def attend_all(queries, keys_cache, own_rows, lengths):
    step_count = own_rows.shape[1]
    cache_pos = lax.broadcasted_iota(jnp.int32, (1, 1, 1, keys_cache.shape[1]), 3)
    cache_ok = cache_pos < lengths.astype(jnp.int32)[:, None, None, None]
    step_here = lax.broadcasted_iota(jnp.int32, (1, step_count, 1, step_count), 1)
    own_here = lax.broadcasted_iota(jnp.int32, (1, step_count, 1, step_count), 3)
    own_ok = own_here <= step_here
    cache_scores = jnp.where(cache_ok, scores_of(queries, keys_cache), -jnp.inf)
    own_scores = jnp.where(own_ok, scores_of(queries, own_rows), -jnp.inf)
    row_top = jnp.maximum(jnp.max(cache_scores, axis=3), jnp.max(own_scores, axis=3))
    cache_exp = jnp.exp(cache_scores - row_top[..., None])
    own_exp = jnp.exp(own_scores - row_top[..., None])
    row_total = jnp.sum(cache_exp, axis=3) + jnp.sum(own_exp, axis=3)
    cache_weights = lax.optimization_barrier(cache_exp.astype(jnp.bfloat16)).astype(jnp.float32)
    own_weights = lax.optimization_barrier(own_exp.astype(jnp.bfloat16)).astype(jnp.float32)
    numerator = jnp.einsum("bshl,bld->bshd", cache_weights, keys_cache[:, :, :LATENT].astype(jnp.float32), precision=lax.Precision.HIGHEST)
    numerator = numerator + jnp.einsum("bshl,bld->bshd", own_weights, own_rows[:, :, :LATENT].astype(jnp.float32), precision=lax.Precision.HIGHEST)
    return numerator / row_total[..., None]


def reference(prompt_cache, prompt_lengths, prompt_replica, new_queries, new_rows, resident_cache, resident_queries, resident_rows, resident_lengths):
    group_count = prompt_cache.shape[0]
    node_count = prompt_cache.shape[1]

    def one_replica(replica_index):
        group_here = replica_index // node_count
        node_here = replica_index % node_count
        source_group = (group_here + group_count - group_count // 2) % group_count
        source_table = prompt_replica[source_group]
        chosen = source_table == node_here
        is_live = jnp.any(chosen, axis=1)
        picked = jnp.argmax(chosen.astype(jnp.int32), axis=1).astype(jnp.int32)
        slot_lengths = jnp.sum(jnp.where(chosen, prompt_lengths[source_group], 0), axis=1).astype(jnp.int32)
        slot_caches = prompt_cache[source_group][jnp.arange(node_count, dtype=jnp.int32), picked]
        context = attend_all(new_queries[group_here, node_here], slot_caches, new_rows[group_here, node_here], slot_lengths)
        context = context * is_live.astype(jnp.float32)[:, None, None, None]
        standing = attend_all(resident_queries[group_here, node_here], resident_cache[group_here, node_here], resident_rows[group_here, node_here], resident_lengths[group_here, node_here])
        return context.astype(jnp.bfloat16), standing.astype(jnp.bfloat16)

    new_all, standing_all = lax.map(one_replica, jnp.arange(group_count * node_count, dtype=jnp.int32))
    new_context = new_all.reshape((group_count, node_count) + new_all.shape[1:])
    resident_context = standing_all.reshape((group_count, node_count) + standing_all.shape[1:])
    return new_context, resident_context
```

```python
import functools

import jax
import jax.numpy as jnp
from jax import lax
from jax.experimental import pallas as pl
from jax.experimental.pallas import tpu as pltpu
from jax.sharding import PartitionSpec as P

LATENT = 512
SCALE = 1.0 / 192.0**0.5
REACH = 2
VMEM_LIMIT = 24 << 20
MESH = pl.DeviceIdType.MESH
NT = (((1,), (1,)), ((), ()))


def dot(a, b, dims=(((1,), (0,)), ((), ()))):
    return lax.dot_general(a, b, dims, preferred_element_type=jnp.float32)


def attend(queries, scores, values, own, step_of_row, finish):
    steps = own.shape[0]
    own32 = own.astype(jnp.float32)
    queries32 = queries.astype(jnp.float32)
    own_scores = []
    for u in range(steps):
        column = jnp.sum(queries32 * own32[u : u + 1], axis=1, keepdims=True) * SCALE
        own_scores.append(jnp.where(step_of_row >= u, column, -jnp.inf))
    top = jnp.max(scores, axis=1, keepdims=True)
    for column in own_scores:
        top = jnp.maximum(top, column)
    weights = jnp.exp(scores - top)
    total = jnp.sum(weights, axis=1, keepdims=True)
    out = values(weights.astype(jnp.bfloat16))
    for u in range(steps):
        weight = jnp.exp(own_scores[u] - top)
        total = total + weight
        out = out + weight.astype(jnp.bfloat16).astype(jnp.float32) * own32[u : u + 1, :LATENT]
    return finish(out, total)


def kernel(
    sizes,
    lengths_hbm,
    replica_hbm,
    resident_lengths_hbm,
    prompt_hbm,
    queries_hbm,
    rows_hbm,
    cache_hbm,
    resident_queries_hbm,
    resident_rows_hbm,
    new_out,
    resident_out,
    lengths_ref,
    replica_ref,
    resident_lengths_ref,
    prompt_ref,
    queries_ref,
    rows_ref,
    cache,
    resident_queries_ref,
    resident_rows_ref,
    stage,
    arrived,
    load_sem,
    cache_sem,
    send_sem,
    relay_sem,
    recv_sem,
):
    groups, nodes, chips = sizes
    group, node, chip = (lax.axis_index(name) for name in ("group", "node", "chip"))
    prompts = prompt_ref.shape[0]
    residents = cache.shape[0]
    steps = rows_ref.shape[1]
    target = lax.rem(group + groups // 2, groups)
    origin = lax.rem(group + groups - groups // 2, groups)
    xor = nodes & (nodes - 1) == 0
    order = tuple(reversed(range(nodes)))
    steps_out = tuple(d for r in range(min(REACH, chips - 1), 0, -1) for d in (r, -r)) + (0,)

    def target_of(a):
        return node ^ a if xor else lax.rem(node + a, nodes)

    def slot_of(a):
        return node ^ a if xor else lax.rem(node + nodes - a, nodes)

    def inside(c):
        return (c >= 0) & (c < chips)

    def direct(source, d):
        return inside(source + d)

    relay_steps = tuple(
        (e, towards) for e in range(REACH, chips - 1) for towards in (1, -1)
    )

    def relays_on(e, towards):
        return inside(chip - towards * e) & inside(chip + towards)

    barrier = pltpu.get_barrier_semaphore()
    for a in range(nodes):
        for d in steps_out:

            @pl.when(inside(chip - d))
            def _(a=a, d=d):
                pl.semaphore_signal(
                    barrier,
                    inc=1,
                    device_id=(origin, slot_of(a), chip - d),
                    device_id_type=MESH,
                )

    expected = 0
    for d in steps_out:
        expected = expected + jnp.where(direct(chip, d), nodes, 0)
    for towards in (1, -1):
        if any(t == towards for _, t in relay_steps):
            e = REACH

            @pl.when(inside(chip - towards) & inside(chip - towards - towards * e))
            def _(towards=towards):
                pl.semaphore_signal(
                    barrier, inc=1, device_id=(group, node, chip - towards), device_id_type=MESH
                )

            expected = expected + jnp.where(relays_on(e, towards), 1, 0)

    pairs = (
        (replica_hbm, replica_ref),
        (prompt_hbm, prompt_ref),
        (resident_queries_hbm, resident_queries_ref),
        (resident_rows_hbm, resident_rows_ref),
        (resident_lengths_hbm, resident_lengths_ref),
        (queries_hbm, queries_ref),
        (rows_hbm, rows_ref),
        (lengths_hbm, lengths_ref),
    )
    loads = [pltpu.make_async_copy(src, dst, load_sem.at[i]) for i, (src, dst) in enumerate(pairs)]
    cache_loads = [
        pltpu.make_async_copy(cache_hbm.at[r], cache.at[r], cache_sem.at[r])
        for r in range(residents)
    ]
    for load in loads[:5] + cache_loads + loads[5:]:
        load.start()

    loads[0].wait()
    loads[1].wait()
    for a in range(nodes):
        replica = target_of(a)
        pick = 0
        for i in range(prompts):
            pick = jnp.where(replica_ref[group, node, i] == replica, i, pick)
        stage[a] = prompt_ref[pick]

    pl.semaphore_wait(barrier, expected)

    def transfer(a, d):
        return pltpu.make_async_remote_copy(
            src_ref=stage.at[a],
            dst_ref=arrived.at[node, chip],
            send_sem=send_sem.at[a, d + chips - 1],
            recv_sem=recv_sem.at[node, chip],
            device_id=(target, target_of(a), chip + d),
            device_id_type=MESH,
        )

    def relay(a, e, towards):
        slot = slot_of(a)
        source = chip - towards * e
        return pltpu.make_async_remote_copy(
            src_ref=arrived.at[slot, source],
            dst_ref=arrived.at[slot, source],
            send_sem=relay_sem.at[a, e, (1 - towards) // 2],
            recv_sem=recv_sem.at[slot, source],
            device_id=(group, node, chip + towards),
            device_id_type=MESH,
        )

    def arrival(slot, source):
        return pltpu.make_async_remote_copy(
            src_ref=stage.at[0],
            dst_ref=arrived.at[slot, source],
            send_sem=send_sem.at[0, 0],
            recv_sem=recv_sem.at[slot, source],
            device_id=(target, node, chip),
            device_id_type=MESH,
        )

    for a in order:
        for d in steps_out:

            @pl.when(direct(chip, d))
            def _(a=a, d=d):
                transfer(a, d).start()

    query_rows = queries_ref.shape[1]
    step_of_row = lax.broadcasted_iota(jnp.int32, (query_rows, 1), 0) // (query_rows // steps)

    def pass_on(a):
        for e, towards in relay_steps:

            @pl.when(relays_on(e, towards))
            def _(e=e, towards=towards):
                arrival(slot_of(a), chip - towards * e).wait_recv()
                relay(a, e, towards).start()

    def resident(r):
        cache_loads[r].wait()
        queries = resident_queries_ref[r]
        scores = dot(queries, cache[r]) * SCALE
        position = lax.broadcasted_iota(jnp.int32, scores.shape, 1)
        scores = jnp.where(position < resident_lengths_ref[r], scores, -jnp.inf)
        resident_out[r] = attend(
            queries,
            scores,
            lambda weights: dot(weights, cache[r, :LATENT], NT),
            resident_rows_ref[r],
            step_of_row,
            lambda out, total: (out / total).astype(resident_out.dtype),
        )

    for load in loads[2:5]:
        load.wait()
    for r in range(residents):
        resident(r)
    for a in order:
        pass_on(a)

    for load in loads[5:]:
        load.wait()
    for a in order:
        s = slot_of(a)
        length = 0
        live = 0
        for i in range(prompts):
            here = replica_ref[origin, s, i] == node
            length = length + jnp.where(here, lengths_ref[origin, s, i], 0)
            live = live + jnp.where(here, 1, 0)
        arrival(s, chip).wait_recv()
        for e in range(1, chips):
            for towards in (1, -1):
                source = chip - towards * e
                here = inside(source)
                if (e, towards) in relay_steps:
                    here = here & jnp.logical_not(inside(chip + towards))

                @pl.when(here)
                def _(s=s, source=source):
                    arrival(s, source).wait_recv()

        tiles = arrived[s].astype(jnp.float32)
        keys = tiles.reshape(-1, tiles.shape[-1]).astype(jnp.bfloat16)
        queries = queries_ref[s]
        scores = dot(queries, keys, NT) * SCALE
        position = lax.broadcasted_iota(jnp.int32, scores.shape, 1)
        scores = jnp.where(position < length, scores, -jnp.inf)
        live32 = jnp.where(live > 0, 1.0, 0.0).astype(jnp.float32)
        new_out[s] = attend(
            queries,
            scores,
            lambda weights, keys=keys: dot(weights, keys[:, :LATENT]),
            rows_ref[s],
            step_of_row,
            lambda out, total, live32=live32: (out / total * live32).astype(new_out.dtype),
        )

    for a in order:
        for d in steps_out:

            @pl.when(direct(chip, d))
            def _(a=a, d=d):
                transfer(a, d).wait_send()

        for e, towards in relay_steps:

            @pl.when(relays_on(e, towards))
            def _(a=a, e=e, towards=towards):
                relay(a, e, towards).wait_send()


def write_out(new_ref, resident_ref, new_out, resident_out, sem):
    copies = [
        pltpu.make_async_copy(new_ref, new_out, sem.at[0]),
        pltpu.make_async_copy(resident_ref, resident_out, sem.at[1]),
    ]
    for copy in copies:
        copy.start()
    for copy in copies:
        copy.wait()


def on_device(
    sizes,
    prompt_cache,
    prompt_lengths,
    prompt_replica,
    new_queries,
    new_rows,
    resident_cache,
    resident_queries,
    resident_rows,
    resident_lengths,
):
    groups, nodes, chips = sizes
    prompts, rows, width = prompt_cache.shape[2:]
    residents, length = resident_cache.shape[2:4]
    steps, heads = new_queries.shape[3:5]
    vmem = pl.BlockSpec(memory_space=pltpu.VMEM)
    tiles = (rows // 8, 8, width)
    any_space = pl.BlockSpec(memory_space=pl.ANY)
    outs = (
        jax.ShapeDtypeStruct((nodes, steps * heads, LATENT), jnp.bfloat16),
        jax.ShapeDtypeStruct((residents, steps * heads, LATENT), jnp.bfloat16),
    )
    operands = (
        prompt_lengths,
        prompt_replica,
        resident_lengths.reshape(residents),
        prompt_cache.reshape((prompts,) + tiles),
        new_queries.reshape(nodes, steps * heads, width),
        new_rows.reshape(nodes, steps, width),
        jnp.swapaxes(resident_cache.reshape(residents, length, width), 1, 2),
        resident_queries.reshape(residents, steps * heads, width),
        resident_rows.reshape(residents, steps, width),
    )
    held = [
        (pltpu.VMEM if jnp.issubdtype(x.dtype, jnp.floating) else pltpu.SMEM)(x.shape, x.dtype)
        for x in operands
    ]
    contexts = pl.pallas_call(
        functools.partial(kernel, sizes),
        out_shape=outs,
        in_specs=[pl.BlockSpec(memory_space=pltpu.HBM)] * len(operands),
        out_specs=(vmem, vmem),
        scratch_shapes=held
        + [
            pltpu.VMEM((nodes,) + tiles, jnp.bfloat16),
            pltpu.VMEM((nodes, chips) + tiles, jnp.bfloat16),
            pltpu.SemaphoreType.DMA((len(operands) - 1,)),
            pltpu.SemaphoreType.DMA((residents,)),
            pltpu.SemaphoreType.DMA((nodes, 2 * chips - 1)),
            pltpu.SemaphoreType.DMA((nodes, chips, 2)),
            pltpu.SemaphoreType.DMA((nodes, chips)),
        ],
        compiler_params=pltpu.CompilerParams(
            collective_id=0, has_side_effects=True, vmem_limit_bytes=VMEM_LIMIT
        ),
        name="handoff",
    )(*[pltpu.with_memory_space_constraint(x, pltpu.HBM) for x in operands])
    new_context, resident_context = pl.pallas_call(
        write_out,
        out_shape=outs,
        in_specs=[any_space] * 2,
        out_specs=(pl.BlockSpec(memory_space=pltpu.HBM),) * 2,
        scratch_shapes=[pltpu.SemaphoreType.DMA((2,))],
        compiler_params=pltpu.CompilerParams(vmem_limit_bytes=1 << 20),
        name="write_out",
    )(*contexts)
    return (
        new_context.reshape(1, 1, nodes, steps, heads, LATENT),
        resident_context.reshape(1, 1, residents, steps, heads, LATENT),
    )


def solution(mesh):
    sizes = tuple(mesh.shape[name] for name in ("group", "node", "chip"))
    in_specs = (
        P("group", "node", None, "chip", None),
        P(),
        P(),
        P("group", "node", None, None, "chip", None),
        P("group", "node", None, None, None),
        P("group", "node", None, None, None),
        P("group", "node", None, None, "chip", None),
        P("group", "node", None, None, None),
        P("group", "node", None),
    )
    out_specs = (
        P("group", "node", None, None, "chip", None),
        P("group", "node", None, None, "chip", None),
    )
    return jax.shard_map(
        functools.partial(on_device, sizes),
        mesh=mesh,
        in_specs=in_specs,
        out_specs=out_specs,
        check_vma=False,
    )
```

```python
import functools

import jax
import jax.numpy as jnp
from jax import lax
from jax.experimental import pallas as pl
from jax.experimental.pallas import tpu as pltpu
from jax.sharding import PartitionSpec as P

LATENT = 512
LANES = 128
SCALE = 1.0 / 192.0**0.5
VMEM_LIMIT = 24 << 20
MESH = pl.DeviceIdType.MESH
NT = (((1,), (1,)), ((), ()))


def dot(a, b, dims=(((1,), (0,)), ((), ()))):
    return lax.dot_general(a, b, dims, preferred_element_type=jnp.float32)


def attend(queries, scores, values, own, step_of_row, finish):
    steps = own.shape[0]
    own32 = own.astype(jnp.float32)
    queries32 = queries.astype(jnp.float32)
    own_scores = []
    for u in range(steps):
        column = jnp.sum(queries32 * own32[u : u + 1], axis=1, keepdims=True) * SCALE
        own_scores.append(jnp.where(step_of_row >= u, column, -jnp.inf))
    top = jnp.max(scores, axis=1, keepdims=True)
    for column in own_scores:
        top = jnp.maximum(top, column)
    weights = jnp.exp(scores - top)
    total = jnp.sum(weights, axis=1, keepdims=True)
    out = values(weights.astype(jnp.bfloat16))
    for u in range(steps):
        weight = jnp.exp(own_scores[u] - top)
        total = total + weight
        out = out + weight.astype(jnp.bfloat16).astype(jnp.float32) * own32[u : u + 1, :LATENT]
    return finish(out, total)


def tile_counts(bands, width):
    across = LATENT // LANES
    share = LANES // (width - LATENT)
    return across, share, bands * across + -(-bands // share)


def pack(prompt_ref, pick, stage, a):
    bands, band, width = prompt_ref.shape[1:]
    across, share, count = tile_counts(bands, width)
    for g in range(bands):
        for c in range(across):
            stage[a, g * across + c] = prompt_ref[pick, g, :, c * LANES : (c + 1) * LANES]
    for i in range(count - bands * across):
        tails = [
            prompt_ref[pick, g, :, LATENT:width].astype(jnp.float32)
            for g in range(i * share, min(bands, (i + 1) * share))
        ]
        tails += [jnp.zeros_like(tails[0])] * (share - len(tails))
        stage[a, bands * across + i] = jnp.concatenate(tails, axis=1).astype(stage.dtype)


def unpack(tiles, bands, band, width):
    across, share, count = tile_counts(bands, width)
    chips = tiles.shape[0]
    rows = chips * bands * band
    latent = tiles[:, : bands * across].reshape(chips, bands, across, band, LANES)
    columns = [latent[:, :, c].reshape(rows, LANES) for c in range(across)]
    tails = []
    for k in range(chips):
        for g in range(bands):
            tile = tiles[k, bands * across + g // share]
            at = g % share * (width - LATENT)
            tails.append(pltpu.roll(tile, LANES - at, 1) if at else tile)
    columns.append(jnp.concatenate(tails, axis=0)[:, : width - LATENT])
    return jnp.concatenate(columns, axis=1).astype(jnp.bfloat16)


def kernel(
    sizes,
    lengths_hbm,
    replica_hbm,
    resident_lengths_hbm,
    prompt_hbm,
    queries_hbm,
    rows_hbm,
    cache_hbm,
    resident_queries_hbm,
    resident_rows_hbm,
    new_out,
    resident_out,
    lengths_ref,
    replica_ref,
    resident_lengths_ref,
    prompt_ref,
    queries_ref,
    rows_ref,
    cache,
    resident_queries_ref,
    resident_rows_ref,
    stage,
    arrived,
    load_sem,
    cache_sem,
    send_sem,
    relay_sem,
    recv_sem,
    ready,
):
    groups, nodes, chips = sizes
    group, node, chip = (lax.axis_index(name) for name in ("group", "node", "chip"))
    prompts = prompt_ref.shape[0]
    residents = cache.shape[0]
    steps = rows_ref.shape[1]
    target = lax.rem(group + groups // 2, groups)
    origin = lax.rem(group + groups - groups // 2, groups)
    xor = nodes & (nodes - 1) == 0
    order = tuple(reversed(range(nodes)))
    def target_of(a):
        return node ^ a if xor else lax.rem(node + a, nodes)

    def slot_of(a):
        return node ^ a if xor else lax.rem(node + nodes - a, nodes)

    line = range(chips)

    def direct(s, t):
        return abs(t - s) <= 2 if s > t else abs(t - s) == 1 or s == 0

    def relays_of(c):
        found = [(s, 1) for s in line[: c + 1] if c + 1 < chips and not direct(s, c + 1)]
        return found + [(s, -1) for s in line[c:] if c > 0 and not direct(s, c - 1)]

    def sends_of(c):
        return [t - c for t in line if t != c and direct(c, t)]

    def at_chip(body):
        for c in line:
            pl.when(chip == c)(functools.partial(body, c))

    def linked(low, high):
        return direct(low, high) or direct(high, low)

    def relay_link(low):
        up = any(way == 1 for _, way in relays_of(low))
        return up or any(way == -1 for _, way in relays_of(low + 1))

    peers = (target,) if groups % 2 == 0 else (target, origin)
    barrier = pltpu.get_barrier_semaphore()

    def tell(sem, to):
        pl.semaphore_signal(sem, inc=1, device_id=to, device_id_type=MESH)

    def enter(c):
        for high in reversed(line[c + 1 :]):
            if linked(c, high):
                for peer in peers:
                    for a in order:
                        tell(barrier, (peer, slot_of(a), high))
        if c + 1 < chips and relay_link(c):
            tell(barrier, (group, node, c + 1))
        for a in order:
            tell(barrier, (origin, slot_of(a), c))

    def entered(c):
        expected = nodes + nodes * len(peers) * sum(linked(low, c) for low in line[:c])
        expected += 1 if c > 0 and relay_link(c - 1) else 0
        pl.semaphore_wait(barrier, expected)
        for low in line[:c]:
            if direct(low, c):
                for a in order:
                    tell(ready.at[c - low], (origin, slot_of(a), low))
        if c > 0 and any(way == 1 for _, way in relays_of(c - 1)):
            tell(ready.at[0], (group, node, c - 1))

    at_chip(enter)

    pairs = (
        (replica_hbm, replica_ref),
        (prompt_hbm, prompt_ref),
        (resident_queries_hbm, resident_queries_ref),
        (resident_rows_hbm, resident_rows_ref),
        (resident_lengths_hbm, resident_lengths_ref),
        (queries_hbm, queries_ref),
        (rows_hbm, rows_ref),
        (lengths_hbm, lengths_ref),
    )
    loads = [pltpu.make_async_copy(src, dst, load_sem.at[i]) for i, (src, dst) in enumerate(pairs)]
    cache_loads = [
        pltpu.make_async_copy(cache_hbm.at[r], cache.at[r], cache_sem.at[r])
        for r in range(residents)
    ]
    for load in loads[:5] + cache_loads + loads[5:]:
        load.start()

    at_chip(entered)
    loads[0].wait()
    loads[1].wait()
    for a in range(nodes):
        replica = target_of(a)
        pick = 0
        for i in range(prompts):
            pick = jnp.where(replica_ref[group, node, i] == replica, i, pick)
        pack(prompt_ref, pick, stage, a)

    def transfer(a, d):
        return pltpu.make_async_remote_copy(
            src_ref=stage.at[a],
            dst_ref=arrived.at[node, chip],
            send_sem=send_sem.at[a, d + chips - 1],
            recv_sem=recv_sem.at[node, chip],
            device_id=(target, target_of(a), chip + d),
            device_id_type=MESH,
        )

    def relay(a, source, way):
        slot = slot_of(a)
        return pltpu.make_async_remote_copy(
            src_ref=arrived.at[slot, source],
            dst_ref=arrived.at[slot, source],
            send_sem=relay_sem.at[a, source],
            recv_sem=recv_sem.at[slot, source],
            device_id=(group, node, chip + way),
            device_id_type=MESH,
        )

    def arrival(slot, source):
        return pltpu.make_async_remote_copy(
            src_ref=stage.at[0],
            dst_ref=arrived.at[slot, source],
            send_sem=send_sem.at[0, 0],
            recv_sem=recv_sem.at[slot, source],
            device_id=(target, node, chip),
            device_id_type=MESH,
        )

    def later(c, d):
        return c == chips - 2 and d == -1

    def send(c):
        for d in sorted(d for d in sends_of(c) if d < 0 and not later(c, d)):
            for a in order:
                transfer(a, d).start()
        for a in order:
            transfer(a, 0).start()
        for d in [d for d in sends_of(c) if d > 0]:
            pl.semaphore_wait(ready.at[d], nodes)
            for a in order:
                transfer(a, d).start()

    def send_later(c):
        for d in sends_of(c):
            if later(c, d):
                for a in order:
                    transfer(a, d).start()

    at_chip(send)

    query_rows = queries_ref.shape[1]
    step_of_row = lax.broadcasted_iota(jnp.int32, (query_rows, 1), 0) // (query_rows // steps)

    def pass_on(c):
        if any(way == 1 for _, way in relays_of(c)):
            pl.semaphore_wait(ready.at[0], 1)
        for a in order:
            for source, way in relays_of(c):
                arrival(slot_of(a), source).wait_recv()
                relay(a, source, way).start()

    def resident(r):
        cache_loads[r].wait()
        queries = resident_queries_ref[r]
        scores = dot(queries, cache[r]) * SCALE
        position = lax.broadcasted_iota(jnp.int32, scores.shape, 1)
        scores = jnp.where(position < resident_lengths_ref[r], scores, -jnp.inf)
        resident_out[r] = attend(
            queries,
            scores,
            lambda weights: dot(weights, cache[r, :LATENT], NT),
            resident_rows_ref[r],
            step_of_row,
            lambda out, total: (out / total).astype(resident_out.dtype),
        )

    for load in loads[2:5]:
        load.wait()
    for r in range(residents):
        resident(r)
        if r == 1:
            at_chip(send_later)
    at_chip(pass_on)

    for load in loads[5:]:
        load.wait()
    for a in order:
        s = slot_of(a)
        length = 0
        live = 0
        for i in range(prompts):
            here = replica_ref[origin, s, i] == node
            length = length + jnp.where(here, lengths_ref[origin, s, i], 0)
            live = live + jnp.where(here, 1, 0)

        def settle(c, s=s):
            passed = [source for source, _ in relays_of(c)]
            for source in line:
                if source not in passed:
                    arrival(s, source).wait_recv()

        at_chip(settle)
        keys = unpack(arrived[s].astype(jnp.float32), *prompt_ref.shape[1:])
        queries = queries_ref[s]
        scores = dot(queries, keys, NT) * SCALE
        position = lax.broadcasted_iota(jnp.int32, scores.shape, 1)
        scores = jnp.where(position < length, scores, -jnp.inf)
        live32 = jnp.where(live > 0, 1.0, 0.0).astype(jnp.float32)
        new_out[s] = attend(
            queries,
            scores,
            lambda weights, keys=keys: dot(weights, keys[:, :LATENT]),
            rows_ref[s],
            step_of_row,
            lambda out, total, live32=live32: (out / total * live32).astype(new_out.dtype),
        )

    def drain(c):
        for a in order:
            for d in sends_of(c) + [0]:
                transfer(a, d).wait_send()
            for source, way in relays_of(c):
                relay(a, source, way).wait_send()

    at_chip(drain)


def write_out(new_ref, resident_ref, new_out, resident_out, sem):
    copies = [
        pltpu.make_async_copy(new_ref, new_out, sem.at[0]),
        pltpu.make_async_copy(resident_ref, resident_out, sem.at[1]),
    ]
    for copy in copies:
        copy.start()
    for copy in copies:
        copy.wait()


def on_device(
    sizes,
    prompt_cache,
    prompt_lengths,
    prompt_replica,
    new_queries,
    new_rows,
    resident_cache,
    resident_queries,
    resident_rows,
    resident_lengths,
):
    groups, nodes, chips = sizes
    prompts, rows, width = prompt_cache.shape[2:]
    residents, length = resident_cache.shape[2:4]
    steps, heads = new_queries.shape[3:5]
    vmem = pl.BlockSpec(memory_space=pltpu.VMEM)
    tiles = (rows // 8, 8, width)
    packed = (tile_counts(rows // 8, width)[2], 8, LANES)
    any_space = pl.BlockSpec(memory_space=pl.ANY)
    outs = (
        jax.ShapeDtypeStruct((nodes, steps * heads, LATENT), jnp.bfloat16),
        jax.ShapeDtypeStruct((residents, steps * heads, LATENT), jnp.bfloat16),
    )
    operands = (
        prompt_lengths,
        prompt_replica,
        resident_lengths.reshape(residents),
        prompt_cache.reshape((prompts,) + tiles),
        new_queries.reshape(nodes, steps * heads, width),
        new_rows.reshape(nodes, steps, width),
        jnp.swapaxes(resident_cache.reshape(residents, length, width), 1, 2),
        resident_queries.reshape(residents, steps * heads, width),
        resident_rows.reshape(residents, steps, width),
    )
    held = [
        (pltpu.VMEM if jnp.issubdtype(x.dtype, jnp.floating) else pltpu.SMEM)(x.shape, x.dtype)
        for x in operands
    ]
    contexts = pl.pallas_call(
        functools.partial(kernel, sizes),
        out_shape=outs,
        in_specs=[pl.BlockSpec(memory_space=pltpu.HBM)] * len(operands),
        out_specs=(vmem, vmem),
        scratch_shapes=held
        + [
            pltpu.VMEM((nodes,) + packed, jnp.bfloat16),
            pltpu.VMEM((nodes, chips) + packed, jnp.bfloat16),
            pltpu.SemaphoreType.DMA((len(operands) - 1,)),
            pltpu.SemaphoreType.DMA((residents,)),
            pltpu.SemaphoreType.DMA((nodes, 2 * chips - 1)),
            pltpu.SemaphoreType.DMA((nodes, chips)),
            pltpu.SemaphoreType.DMA((nodes, chips)),
            pltpu.SemaphoreType.REGULAR((chips,)),
        ],
        compiler_params=pltpu.CompilerParams(
            collective_id=0, has_side_effects=True, vmem_limit_bytes=VMEM_LIMIT
        ),
        name="handoff",
    )(*[pltpu.with_memory_space_constraint(x, pltpu.HBM) for x in operands])
    new_context, resident_context = pl.pallas_call(
        write_out,
        out_shape=outs,
        in_specs=[any_space] * 2,
        out_specs=(pl.BlockSpec(memory_space=pltpu.HBM),) * 2,
        scratch_shapes=[pltpu.SemaphoreType.DMA((2,))],
        compiler_params=pltpu.CompilerParams(vmem_limit_bytes=1 << 20),
        name="write_out",
    )(*contexts)
    return (
        new_context.reshape(1, 1, nodes, steps, heads, LATENT),
        resident_context.reshape(1, 1, residents, steps, heads, LATENT),
    )


def solution(mesh):
    sizes = tuple(mesh.shape[name] for name in ("group", "node", "chip"))
    in_specs = (
        P("group", "node", None, "chip", None),
        P(),
        P(),
        P("group", "node", None, None, "chip", None),
        P("group", "node", None, None, None),
        P("group", "node", None, None, None),
        P("group", "node", None, None, "chip", None),
        P("group", "node", None, None, None),
        P("group", "node", None),
    )
    out_specs = (
        P("group", "node", None, None, "chip", None),
        P("group", "node", None, None, "chip", None),
    )
    return jax.shard_map(
        functools.partial(on_device, sizes),
        mesh=mesh,
        in_specs=in_specs,
        out_specs=out_specs,
        check_vma=False,
    )
```

```python
import functools

import jax
import jax.numpy as jnp
from jax import lax
from jax.experimental import pallas as pl
from jax.experimental.pallas import tpu as pltpu
from jax.sharding import PartitionSpec as P

LATENT = 512
LANES = 128
SCALE = 1.0 / 192.0**0.5
VMEM_LIMIT = 24 << 20
MESH = pl.DeviceIdType.MESH
NT = (((1,), (1,)), ((), ()))


def dot(a, b, dims=(((1,), (0,)), ((), ()))):
    return lax.dot_general(a, b, dims, preferred_element_type=jnp.float32)


def attend(queries, scores, values, own, step_of_row, finish):
    steps = own.shape[0]
    own32 = own.astype(jnp.float32)
    queries32 = queries.astype(jnp.float32)
    own_scores = []
    for u in range(steps):
        column = jnp.sum(queries32 * own32[u : u + 1], axis=1, keepdims=True) * SCALE
        own_scores.append(jnp.where(step_of_row >= u, column, -jnp.inf))
    top = jnp.max(scores, axis=1, keepdims=True)
    for column in own_scores:
        top = jnp.maximum(top, column)
    weights = jnp.exp(scores - top)
    total = jnp.sum(weights, axis=1, keepdims=True)
    out = values(weights.astype(jnp.bfloat16))
    for u in range(steps):
        weight = jnp.exp(own_scores[u] - top)
        total = total + weight
        out = out + weight.astype(jnp.bfloat16).astype(jnp.float32) * own32[u : u + 1, :LATENT]
    return finish(out, total)


def tile_counts(bands, width):
    across = LATENT // LANES
    share = LANES // (width - LATENT)
    return across, share, bands * across + -(-bands // share)


def pack(prompt_ref, pick, stage, a):
    bands, band, width = prompt_ref.shape[1:]
    across, share, count = tile_counts(bands, width)
    for g in range(bands):
        for c in range(across):
            stage[a, g * across + c] = prompt_ref[pick, g, :, c * LANES : (c + 1) * LANES]
    for i in range(count - bands * across):
        tails = [
            prompt_ref[pick, g, :, LATENT:width].astype(jnp.float32)
            for g in range(i * share, min(bands, (i + 1) * share))
        ]
        tails += [jnp.zeros_like(tails[0])] * (share - len(tails))
        stage[a, bands * across + i] = jnp.concatenate(tails, axis=1).astype(stage.dtype)


def unpack(tiles, bands, band, width):
    across, share, count = tile_counts(bands, width)
    chips = tiles.shape[0]
    rows = chips * bands * band
    latent = tiles[:, : bands * across].reshape(chips, bands, across, band, LANES)
    columns = [latent[:, :, c].reshape(rows, LANES) for c in range(across)]
    tails = []
    for k in range(chips):
        for g in range(bands):
            tile = tiles[k, bands * across + g // share]
            at = g % share * (width - LATENT)
            tails.append(pltpu.roll(tile, LANES - at, 1) if at else tile)
    columns.append(jnp.concatenate(tails, axis=0)[:, : width - LATENT])
    return jnp.concatenate(columns, axis=1).astype(jnp.bfloat16)


def kernel(
    sizes,
    lengths_hbm,
    replica_hbm,
    resident_lengths_hbm,
    prompt_hbm,
    queries_hbm,
    rows_hbm,
    cache_hbm,
    resident_queries_hbm,
    resident_rows_hbm,
    new_out,
    resident_out,
    lengths_ref,
    replica_ref,
    resident_lengths_ref,
    prompt_ref,
    queries_ref,
    rows_ref,
    cache,
    resident_queries_ref,
    resident_rows_ref,
    stage,
    arrived,
    load_sem,
    cache_sem,
    send_sem,
    relay_sem,
    recv_sem,
    ready,
    plane,
):
    groups, nodes, chips = sizes
    group, node, chip = (lax.axis_index(name) for name in ("group", "node", "chip"))
    prompts = prompt_ref.shape[0]
    residents = cache.shape[0]
    steps = rows_ref.shape[1]
    target = lax.rem(group + groups // 2, groups)
    origin = lax.rem(group + groups - groups // 2, groups)
    xor = nodes & (nodes - 1) == 0
    order = tuple(range(nodes))
    def target_of(a):
        return node ^ a if xor else lax.rem(node + a, nodes)

    def slot_of(a):
        return node ^ a if xor else lax.rem(node + nodes - a, nodes)

    split = xor and groups % 2 == 0
    line = range(chips)

    def direct(s, t, a):
        return abs(t - s) <= 2 if s > t else (abs(t - s) == 1 or s == 0)

    def relays_of(c, a):
        found = [(s, 1) for s in line[: c + 1] if c + 1 < chips and not direct(s, c + 1, a)]
        return found + [(s, -1) for s in line[c:] if c > 0 and not direct(s, c - 1, a)]

    def relays_any(c, way):
        return any(w == way for a in order for _, w in relays_of(c, a))

    def sends_of(c, a):
        return [t - c for t in line if t != c and direct(c, t, a)]

    def at_chip(body):
        for c in line:
            pl.when(chip == c)(functools.partial(body, c))

    def linked(low, high):
        return any(direct(low, high, a) or direct(high, low, a) for a in order)

    def relay_link(low):
        return relays_any(low, 1) or relays_any(low + 1, -1)

    peers = (target,) if groups % 2 == 0 else (target, origin)
    barrier = pltpu.get_barrier_semaphore()

    def tell(sem, to):
        pl.semaphore_signal(sem, inc=1, device_id=to, device_id_type=MESH)

    def enter(c):
        for high in reversed(line[c + 1 :]):
            if linked(c, high):
                for peer in peers:
                    for a in order:
                        tell(barrier, (peer, slot_of(a), high))
        if c + 1 < chips and relay_link(c):
            tell(barrier, (group, node, c + 1))
        for a in order:
            if split and a > 0:
                pl.when(slot_of(a) > node)(
                    functools.partial(tell, barrier, (origin, slot_of(a), c))
                )
            else:
                tell(barrier, (origin, slot_of(a), c))

    def entered(c):
        expected = (node + 1 if split else nodes) + nodes * len(peers) * sum(linked(low, c) for low in line[:c])
        expected += 1 if c > 0 and relay_link(c - 1) else 0
        pl.semaphore_wait(barrier, expected)
        for low in line[:c]:
            for a in order:
                if direct(low, c, a):
                    tell(ready.at[c - low], (origin, slot_of(a), low))
        if split:
            for a in order[1:]:
                pl.when(slot_of(a) < node)(
                    functools.partial(tell, plane.at[a], (origin, slot_of(a), c))
                )
        if c > 0 and relays_any(c - 1, 1):
            tell(ready.at[0], (group, node, c - 1))

    at_chip(enter)

    pairs = (
        (replica_hbm, replica_ref),
        (prompt_hbm, prompt_ref),
        (resident_queries_hbm, resident_queries_ref),
        (resident_rows_hbm, resident_rows_ref),
        (resident_lengths_hbm, resident_lengths_ref),
        (queries_hbm, queries_ref),
        (rows_hbm, rows_ref),
        (lengths_hbm, lengths_ref),
    )
    loads = [pltpu.make_async_copy(src, dst, load_sem.at[i]) for i, (src, dst) in enumerate(pairs)]
    cache_loads = [
        pltpu.make_async_copy(cache_hbm.at[r], cache.at[r], cache_sem.at[r])
        for r in range(residents)
    ]
    for load in loads[:5] + cache_loads + loads[5:]:
        load.start()

    at_chip(entered)
    loads[0].wait()
    loads[1].wait()
    for a in range(nodes):
        replica = target_of(a)
        pick = 0
        for i in range(prompts):
            pick = jnp.where(replica_ref[group, node, i] == replica, i, pick)
        pack(prompt_ref, pick, stage, a)

    def transfer(a, d):
        return pltpu.make_async_remote_copy(
            src_ref=stage.at[a],
            dst_ref=arrived.at[node, chip],
            send_sem=send_sem.at[a, d + chips - 1],
            recv_sem=recv_sem.at[node, chip],
            device_id=(target, target_of(a), chip + d),
            device_id_type=MESH,
        )

    def relay(a, source, way):
        slot = slot_of(a)
        return pltpu.make_async_remote_copy(
            src_ref=arrived.at[slot, source],
            dst_ref=arrived.at[slot, source],
            send_sem=relay_sem.at[a, source],
            recv_sem=recv_sem.at[slot, source],
            device_id=(group, node, chip + way),
            device_id_type=MESH,
        )

    def arrival(slot, source):
        return pltpu.make_async_remote_copy(
            src_ref=stage.at[0],
            dst_ref=arrived.at[slot, source],
            send_sem=send_sem.at[0, 0],
            recv_sem=recv_sem.at[slot, source],
            device_id=(target, node, chip),
            device_id_type=MESH,
        )

    def later(c, d):
        return c == chips - 2 and d == -1

    def send(c):
        for d in range(-c, 0):
            for a in order:
                if d in sends_of(c, a) and not later(c, d):
                    transfer(a, d).start()
        for a in order:
            if split and a > 0:
                pl.when(target_of(a) < node)(transfer(a, 0).start)
            else:
                transfer(a, 0).start()

        def acknowledged(a):
            pl.semaphore_wait(plane.at[a], 1)
            transfer(a, 0).start()

        if split:
            for a in range(1, nodes):
                pl.when(target_of(a) > node)(functools.partial(acknowledged, a))
        for d in range(1, chips - c):
            using = [a for a in order if d in sends_of(c, a)]
            if using:
                pl.semaphore_wait(ready.at[d], len(using))
            for a in using:
                transfer(a, d).start()

    def send_later(c):
        for d in range(-c, 0):
            for a in order:
                if d in sends_of(c, a) and later(c, d):
                    transfer(a, d).start()

    at_chip(send)

    query_rows = queries_ref.shape[1]
    step_of_row = lax.broadcasted_iota(jnp.int32, (query_rows, 1), 0) // (query_rows // steps)

    def pass_on(c):
        if relays_any(c, 1):
            pl.semaphore_wait(ready.at[0], 1)
        for a in order:
            for source, way in relays_of(c, a):
                arrival(slot_of(a), source).wait_recv()
                relay(a, source, way).start()

    def resident(r):
        cache_loads[r].wait()
        queries = resident_queries_ref[r]
        scores = dot(queries, cache[r]) * SCALE
        position = lax.broadcasted_iota(jnp.int32, scores.shape, 1)
        scores = jnp.where(position < resident_lengths_ref[r], scores, -jnp.inf)
        resident_out[r] = attend(
            queries,
            scores,
            lambda weights: dot(weights, cache[r, :LATENT], NT),
            resident_rows_ref[r],
            step_of_row,
            lambda out, total: (out / total).astype(resident_out.dtype),
        )

    for load in loads[2:5]:
        load.wait()
    for r in range(residents):
        resident(r)
        if r == 1:
            at_chip(send_later)
    at_chip(pass_on)

    for load in loads[5:]:
        load.wait()
    for a in order:
        s = slot_of(a)
        length = 0
        live = 0
        for i in range(prompts):
            here = replica_ref[origin, s, i] == node
            length = length + jnp.where(here, lengths_ref[origin, s, i], 0)
            live = live + jnp.where(here, 1, 0)

        def settle(c, s=s, a=a):
            passed = [source for source, _ in relays_of(c, a)]
            for source in line:
                if source not in passed:
                    arrival(s, source).wait_recv()

        at_chip(settle)
        keys = unpack(arrived[s].astype(jnp.float32), *prompt_ref.shape[1:])
        queries = queries_ref[s]
        scores = dot(queries, keys, NT) * SCALE
        position = lax.broadcasted_iota(jnp.int32, scores.shape, 1)
        scores = jnp.where(position < length, scores, -jnp.inf)
        live32 = jnp.where(live > 0, 1.0, 0.0).astype(jnp.float32)
        new_out[s] = attend(
            queries,
            scores,
            lambda weights, keys=keys: dot(weights, keys[:, :LATENT]),
            rows_ref[s],
            step_of_row,
            lambda out, total, live32=live32: (out / total * live32).astype(new_out.dtype),
        )

    def drain(c):
        for a in order:
            for d in sends_of(c, a) + [0]:
                transfer(a, d).wait_send()
            for source, way in relays_of(c, a):
                relay(a, source, way).wait_send()

    at_chip(drain)


def write_out(new_ref, resident_ref, new_out, resident_out, sem):
    copies = [
        pltpu.make_async_copy(new_ref, new_out, sem.at[0]),
        pltpu.make_async_copy(resident_ref, resident_out, sem.at[1]),
    ]
    for copy in copies:
        copy.start()
    for copy in copies:
        copy.wait()


def on_device(
    sizes,
    prompt_cache,
    prompt_lengths,
    prompt_replica,
    new_queries,
    new_rows,
    resident_cache,
    resident_queries,
    resident_rows,
    resident_lengths,
):
    groups, nodes, chips = sizes
    prompts, rows, width = prompt_cache.shape[2:]
    residents, length = resident_cache.shape[2:4]
    steps, heads = new_queries.shape[3:5]
    vmem = pl.BlockSpec(memory_space=pltpu.VMEM)
    tiles = (rows // 8, 8, width)
    packed = (tile_counts(rows // 8, width)[2], 8, LANES)
    any_space = pl.BlockSpec(memory_space=pl.ANY)
    outs = (
        jax.ShapeDtypeStruct((nodes, steps * heads, LATENT), jnp.bfloat16),
        jax.ShapeDtypeStruct((residents, steps * heads, LATENT), jnp.bfloat16),
    )
    operands = (
        prompt_lengths,
        prompt_replica,
        resident_lengths.reshape(residents),
        prompt_cache.reshape((prompts,) + tiles),
        new_queries.reshape(nodes, steps * heads, width),
        new_rows.reshape(nodes, steps, width),
        jnp.swapaxes(resident_cache.reshape(residents, length, width), 1, 2),
        resident_queries.reshape(residents, steps * heads, width),
        resident_rows.reshape(residents, steps, width),
    )
    held = [
        (pltpu.VMEM if jnp.issubdtype(x.dtype, jnp.floating) else pltpu.SMEM)(x.shape, x.dtype)
        for x in operands
    ]
    contexts = pl.pallas_call(
        functools.partial(kernel, sizes),
        out_shape=outs,
        in_specs=[pl.BlockSpec(memory_space=pltpu.HBM)] * len(operands),
        out_specs=(vmem, vmem),
        scratch_shapes=held
        + [
            pltpu.VMEM((nodes,) + packed, jnp.bfloat16),
            pltpu.VMEM((nodes, chips) + packed, jnp.bfloat16),
            pltpu.SemaphoreType.DMA((len(operands) - 1,)),
            pltpu.SemaphoreType.DMA((residents,)),
            pltpu.SemaphoreType.DMA((nodes, 2 * chips - 1)),
            pltpu.SemaphoreType.DMA((nodes, chips)),
            pltpu.SemaphoreType.DMA((nodes, chips)),
            pltpu.SemaphoreType.REGULAR((chips,)),
            pltpu.SemaphoreType.REGULAR((nodes,)),
        ],
        compiler_params=pltpu.CompilerParams(
            collective_id=0, has_side_effects=True, vmem_limit_bytes=VMEM_LIMIT
        ),
        name="handoff",
    )(*[pltpu.with_memory_space_constraint(x, pltpu.HBM) for x in operands])
    new_context, resident_context = pl.pallas_call(
        write_out,
        out_shape=outs,
        in_specs=[any_space] * 2,
        out_specs=(pl.BlockSpec(memory_space=pltpu.HBM),) * 2,
        scratch_shapes=[pltpu.SemaphoreType.DMA((2,))],
        compiler_params=pltpu.CompilerParams(vmem_limit_bytes=1 << 20),
        name="write_out",
    )(*contexts)
    return (
        new_context.reshape(1, 1, nodes, steps, heads, LATENT),
        resident_context.reshape(1, 1, residents, steps, heads, LATENT),
    )


def solution(mesh):
    sizes = tuple(mesh.shape[name] for name in ("group", "node", "chip"))
    in_specs = (
        P("group", "node", None, "chip", None),
        P(),
        P(),
        P("group", "node", None, None, "chip", None),
        P("group", "node", None, None, None),
        P("group", "node", None, None, None),
        P("group", "node", None, None, "chip", None),
        P("group", "node", None, None, None),
        P("group", "node", None),
    )
    out_specs = (
        P("group", "node", None, None, "chip", None),
        P("group", "node", None, None, "chip", None),
    )
    return jax.shard_map(
        functools.partial(on_device, sizes),
        mesh=mesh,
        in_specs=in_specs,
        out_specs=out_specs,
        check_vma=False,
    )
```
